32 devices in a mesh: dp: 4 (over y, z), dcp: 8 (over x, core).
Axes of the slice: x: 4, y: 2, z: 2, core: 2. Of those that a mesh axis runs over, the one named last changes fastest.
The devices are a block of a 4x4x8 slice.
Arguments:
- q: bfloat16 [128, 128, 576], P('dp', 'dcp'), parts along dimension 0
- cache: bfloat16 [128, 128, 8, 8, 576], P('dp', None, 'dcp'), parts along dimension 0
- lens: int32 [128], P('dp'), parts along dimension 0
Outputs:
- output: bfloat16 [128, 128, 512], P('dp', 'dcp'), parts along dimension 0
There are 4 independent parts. The reference program is written for one: setup_inputs(seed, part) draws one part's arguments, and reference() takes and returns one part's arrays. A program takes and returns all parts, laid end to end along the dimension named above; each array names one.
All inputs are finite; a program needn't handle non-finite values.
Results may differ from the reference program's by a relative error of at most 0.00740574.
Values are sent between devices in bfloat16 or wider.
A program may use at most 768 MiB of HBM per device.

```python
import jax
import jax.numpy as jnp
from jax import lax

B = 32
S = 8192
PAGE = 8
DCP = 8
HEADS = 128
LORA = 512
ROPE = 64
NOPE = 128

R = S // (PAGE * DCP)
K = LORA + ROPE


def setup_inputs(seed: int = 0, part: int = 0) -> dict:
    key = jax.random.fold_in(jax.random.key(seed), part)
    kq, kc, kl = jax.random.split(key, 3)
    qs = 1.5 * ((NOPE + ROPE) / 2.0) ** 0.5
    scale = jnp.concatenate([jnp.full((LORA,), qs / LORA ** 0.5, jnp.float32), jnp.full((ROPE,), qs / ROPE ** 0.5, jnp.float32)])
    q = (jax.random.normal(kq, (B, HEADS, K), jnp.float32) * scale).astype(jnp.bfloat16)
    cache = jax.random.normal(kc, (B, R, DCP, PAGE, K), jnp.float32).astype(jnp.bfloat16)
    lens = jax.random.randint(kl, (B,), S // 4, S + 1, jnp.int32)
    return {'q': q, 'cache': cache, 'lens': lens}


def reference(q, cache, lens):
    c = cache.reshape(B, S, K)
    pos = jnp.arange(S)

    def one(args):
        qb, cb, lb = args
        s = jnp.dot(qb, cb.T, preferred_element_type=jnp.float32) / (NOPE + ROPE) ** 0.5
        s = jnp.where(pos[None, :] < lb, s, -jnp.inf)
        a = jax.nn.softmax(s, axis=1)
        o = jnp.dot(a, cb[:, :LORA].astype(jnp.float32), preferred_element_type=jnp.float32)
        return o.astype(jnp.bfloat16)

    return lax.map(one, (q, c, lens))
```

```python
import functools

import jax
import jax.numpy as jnp
from jax import lax
from jax.experimental import pallas as pl
from jax.experimental.pallas import tpu as pltpu
from jax.sharding import PartitionSpec as P

ROPE = 64
QK_DIM = 192
C2 = QK_DIM ** -0.5 * 1.4426950408889634

G = 2
AHEAD = 3
RING = 14
PSLOT = 8
LB = 2


def kernel(n, q_hbm, c_hbm, lens_ref, o_ref, qall, cbuf, pbuf, mbuf, lse_all, obuf, xrecv, snd,
           relay_in, o_in, lsem, csem, send_sem, ql_sem, qr_sem, qd_sem, qp_sem, lse_sem, x_sem,
           a_sem, ol_sem, or_sem, od_sem):
    nseq, hl, k = q_hbm.shape
    npage, _, r = c_hbm.shape[1:]
    lorav = k - ROPE
    nx = n // 2
    half = nx * hl
    heads = n * hl
    nc = nseq // G

    me = lax.axis_index('dcp')
    x = me // 2
    core = me % 2
    right = (me + 2) % n
    left = (me + n - 2) % n
    opp = (me + 4) % n
    mate = me + 1 - 2 * core

    def row(j):
        return ((j % 2) * nx + j // 2) * hl

    def remote(src, dst, ssem, rsem, dev):
        return pltpu.make_async_remote_copy(
            src_ref=src, dst_ref=dst, send_sem=ssem, recv_sem=rsem, device_id={'dcp': dev},
            device_id_type=pl.DeviceIdType.MESH)

    def wait_on(ref, sem):
        pltpu.make_async_copy(ref, ref, sem).wait()

    def cache_copy(b):
        s = b % RING
        return pltpu.make_async_copy(c_hbm.at[b], cbuf.at[s], csem.at[s])

    def qblk(c, j):
        return qall.at[pl.ds(c * G, G), pl.ds(row(j), hl), :]

    qcopy = pltpu.make_async_copy(q_hbm, qall.at[:, pl.ds(row(me), hl), :], lsem.at[0])
    qcopy.start()
    for b in range(RING):
        cache_copy(b).start()

    barrier = pltpu.get_barrier_semaphore()
    for d in range(1, n):
        pl.semaphore_signal(barrier, inc=1, device_id={'dcp': (me + d) % n},
                            device_id_type=pl.DeviceIdType.MESH)
    pl.semaphore_wait(barrier, n - 1)
    qcopy.wait()

    def send_own(c):
        blk = qblk(c, me)
        remote(blk, blk, send_sem.at[0], ql_sem.at[c], right).start()
        remote(blk, blk, send_sem.at[1], qr_sem.at[c], left).start()
        remote(blk, blk, send_sem.at[2], qp_sem.at[c], mate).start()

    def q_first(c):
        wait_on(qblk(c, left), ql_sem.at[c])
        wait_on(qblk(c, right), qr_sem.at[c])
        even = c % 2 == 0
        blk = qblk(c, jnp.where(even, left, right))
        remote(blk, blk, send_sem.at[3], qd_sem.at[c], jnp.where(even, right, left)).start()
        for j in (left, right):
            blk = qblk(c, j)
            remote(blk, blk, send_sem.at[2], qp_sem.at[c], mate).start()

    def q_second(c):
        blk = qblk(c, opp)
        wait_on(blk, qd_sem.at[c])
        remote(blk, blk, send_sem.at[2], qp_sem.at[c], mate).start()

    def q_third(c):
        wait_on(qall.at[pl.ds(c * G, G), pl.ds((1 - core) * half, half), :], qp_sem.at[c])

    def cache_t(s):
        return cbuf[s]

    def scores(c):
        for g in range(G):
            b = c * G + g
            cache_copy(b).wait()
            ct = cbuf[b % RING]
            ct = jnp.concatenate([ct[i] for i in range(npage)], axis=1)
            s = lax.dot_general(qall[b], ct, (((1,), (0,)), ((), ())), preferred_element_type=jnp.float32)
            length = lens_ref[b] - me * npage
            posr = lax.broadcasted_iota(jnp.int32, (1, r), 1) * (n * npage)
            mask = jnp.concatenate([posr < length - i for i in range(npage)], axis=1)
            s = jnp.where(mask, s, -jnp.inf)
            m = jnp.max(s, axis=1, keepdims=True) * C2
            msafe = jnp.where(m == -jnp.inf, 0.0, m)
            p = jnp.exp2(s * C2 - msafe)
            l = jnp.sum(p, axis=1, keepdims=True)
            ps = b % PSLOT
            pbuf[ps] = p
            mbuf[ps] = m
            lse = jnp.where(l > 0.0, msafe + jnp.log2(jnp.where(l > 0.0, l, 1.0)), -jnp.inf)
            t = jnp.transpose(jnp.broadcast_to(lse, (heads, heads)))
            lse_all[me, b] = t[0:1]
        blk = lse_all.at[me, pl.ds(c * G, G)]
        for d in range(1, n):
            remote(blk, blk, send_sem.at[4], lse_sem.at[c], (me + d) % n).start()

    def product(c):
        wait_on(lse_all.at[pl.ds(0, n - 1), pl.ds(c * G, G)], lse_sem.at[c])
        for g in range(G):
            b = c * G + g
            rows = [lse_all[j, b] for j in range(n)]
            top = functools.reduce(jnp.maximum, rows)
            tot = functools.reduce(jnp.add, [jnp.exp2(z - top) for z in rows])
            big = top + jnp.log2(tot)
            bigc = jnp.transpose(jnp.broadcast_to(big, (heads, heads)))[:, 0:1]
            ps = b % PSLOT
            f = jnp.exp2(mbuf[ps] - bigc)
            a = (pbuf[ps] * f).astype(jnp.bfloat16)
            ct = cbuf[b % RING]
            ct = jnp.concatenate([ct[i, :lorav] for i in range(npage)], axis=1)
            ot = lax.dot_general(ct, a, (((1,), (1,)), ((), ())), preferred_element_type=jnp.float32)
            obuf[b] = jnp.transpose(ot)
            remote(obuf.at[b, pl.ds((1 - core) * half, half)], xrecv.at[b], send_sem.at[5], x_sem.at[c],
                   mate).start()

            @pl.when(b + RING < nseq)
            def _():
                cache_copy(b + RING).start()

    def chip_sum(c):
        bs = pl.ds(c * G, G)
        wait_on(xrecv.at[bs], x_sem.at[c])
        snd[bs] = (obuf[bs, pl.ds(core * half, half)] + xrecv[bs]).astype(jnp.bfloat16)

        def part(j):
            return snd.at[bs, pl.ds((j // 2) * hl, hl)]

        even = c % 2 == 0
        remote(part(opp), relay_in.at[bs], send_sem.at[6], a_sem.at[c], jnp.where(even, right, left)).start()
        remote(part(right), o_in.at[0, bs], send_sem.at[6], ol_sem.at[c], right).start()
        remote(part(left), o_in.at[1, bs], send_sem.at[6], or_sem.at[c], left).start()

    def relay(c):
        bs = pl.ds(c * G, G)
        wait_on(relay_in.at[bs], a_sem.at[c])
        remote(relay_in.at[bs], o_in.at[2, bs], send_sem.at[7], od_sem.at[c],
               jnp.where(c % 2 == 0, right, left)).start()

    def final(c):
        bs = pl.ds(c * G, G)
        wait_on(o_in.at[0, bs], ol_sem.at[c])
        wait_on(o_in.at[1, bs], or_sem.at[c])
        wait_on(o_in.at[2, bs], od_sem.at[c])
        own = obuf[bs, pl.ds(row(me), hl)] + xrecv[bs, pl.ds(x * hl, hl)]
        o_ref[bs] = (own + o_in[0, bs].astype(jnp.float32) + o_in[1, bs].astype(jnp.float32)
                     + o_in[2, bs].astype(jnp.float32)).astype(o_ref.dtype)

    for c in range(AHEAD):
        send_own(c)

    stages = [(q_first, 0), (q_second, 1), (q_third, 2), (scores, 2), (product, 2 + LB),
              (chip_sum, 3 + LB), (relay, 4 + LB), (final, 6 + LB)]
    last = max(d for _, d in stages)

    @pl.loop(0, nc + last)
    def _(it):
        @pl.when(it + AHEAD < nc)
        def _():
            send_own(it + AHEAD)

        for f, d in stages:
            @pl.when((it >= d) & (it < nc + d))
            def _(f=f, d=d):
                f(it - d)

    wait_on(qall.at[:, pl.ds(0, hl), :], send_sem.at[0])
    wait_on(qall.at[:, pl.ds(0, hl), :], send_sem.at[1])
    wait_on(qall.at[:, pl.ds(0, half), :], send_sem.at[2])
    wait_on(qall.at[:, pl.ds(0, hl), :], send_sem.at[3])
    wait_on(lse_all.at[pl.ds(0, n - 1)], send_sem.at[4])
    wait_on(xrecv, send_sem.at[5])
    wait_on(snd.at[:, pl.ds(0, (nx - 1) * hl)], send_sem.at[6])
    wait_on(relay_in, send_sem.at[7])


def solution(mesh):
    n = mesh.shape['dcp']

    def local(q, cache, lens):
        b, hl, k = q.shape
        r = cache.shape[1]
        page = cache.shape[3]
        lorav = k - ROPE
        ct = cache.reshape(b, r, page, k).transpose(0, 2, 3, 1)
        heads = n * hl
        half = heads // 2
        nc = b // G
        dma = pltpu.SemaphoreType.DMA
        return pl.pallas_call(
            functools.partial(kernel, n),
            out_shape=jax.ShapeDtypeStruct((b, hl, lorav), jnp.bfloat16),
            in_specs=[pl.BlockSpec(memory_space=pl.ANY), pl.BlockSpec(memory_space=pl.ANY),
                      pl.BlockSpec(memory_space=pltpu.SMEM)],
            out_specs=pl.BlockSpec(memory_space=pltpu.VMEM),
            scratch_shapes=[
                pltpu.VMEM((b, heads, k), jnp.bfloat16),
                pltpu.VMEM((RING, page, k, r), jnp.bfloat16),
                pltpu.VMEM((PSLOT, heads, r * page), jnp.float32),
                pltpu.VMEM((PSLOT, heads, 1), jnp.float32),
                pltpu.VMEM((n, b, 1, heads), jnp.float32),
                pltpu.VMEM((b, heads, lorav), jnp.float32),
                pltpu.VMEM((b, half, lorav), jnp.float32),
                pltpu.VMEM((b, half, lorav), jnp.bfloat16),
                pltpu.VMEM((b, hl, lorav), jnp.bfloat16),
                pltpu.VMEM((3, b, hl, lorav), jnp.bfloat16),
                dma((1,)), dma((RING,)), dma((8,)),
            ] + [dma((nc,))] * 10,
            compiler_params=pltpu.CompilerParams(
                collective_id=0, has_side_effects=True, vmem_limit_bytes=66_000_000),
        )(q, ct, lens)

    return jax.shard_map(local, mesh=mesh,
                         in_specs=(P('dp', 'dcp', None), P('dp', None, 'dcp', None, None), P('dp')),
                         out_specs=P('dp', 'dcp', None), check_vma=False)
```

```python
import functools

import jax
import jax.numpy as jnp
from jax import lax
from jax.experimental import pallas as pl
from jax.experimental.pallas import tpu as pltpu
from jax.sharding import PartitionSpec as P

ROPE = 64
QK_DIM = 192
C2 = QK_DIM ** -0.5 * 1.4426950408889634

G = 2
AHEAD = 2
RING = 14
PSLOT = 8
D_Q2 = 2
D_Q3 = 4
D_SC = 4
D_PR = 7
D_CS = 9
D_RL = 12
D_FI = 16
NT = True


def kernel(n, q_hbm, c_hbm, lens_ref, o_ref, qall, cbuf, pbuf, mbuf, lse_all, obuf, xrecv, snd,
           relay_in, o_in, lsem, csem, send_sem, ql_sem, qr_sem, qd_sem, qp_sem, lse_sem, x_sem,
           a_sem, ol_sem, or_sem, od_sem):
    nseq, hl, k = q_hbm.shape
    npage, _, r = c_hbm.shape[1:]
    lorav = k - ROPE
    nx = n // 2
    half = nx * hl
    heads = n * hl
    nc = nseq // G

    me = lax.axis_index('dcp')
    x = me // 2
    core = me % 2
    right = (me + 2) % n
    left = (me + n - 2) % n
    opp = (me + 4) % n
    mate = me + 1 - 2 * core

    def row(j):
        return ((j % 2) * nx + j // 2) * hl

    def remote(src, dst, ssem, rsem, dev):
        return pltpu.make_async_remote_copy(
            src_ref=src, dst_ref=dst, send_sem=ssem, recv_sem=rsem, device_id={'dcp': dev},
            device_id_type=pl.DeviceIdType.MESH)

    def wait_on(ref, sem):
        pltpu.make_async_copy(ref, ref, sem).wait()

    def cache_copy(b):
        s = b % RING
        return pltpu.make_async_copy(c_hbm.at[b], cbuf.at[s], csem.at[s])

    def qblk(c, j):
        return qall.at[pl.ds(c * G, G), pl.ds(row(j), hl), :]

    qcopy = pltpu.make_async_copy(q_hbm, qall.at[:, pl.ds(row(me), hl), :], lsem.at[0])
    qcopy.start()
    for b in range(RING):
        cache_copy(b).start()

    barrier = pltpu.get_barrier_semaphore()
    for d in range(1, n):
        pl.semaphore_signal(barrier, inc=1, device_id={'dcp': (me + d) % n},
                            device_id_type=pl.DeviceIdType.MESH)
    pl.semaphore_wait(barrier, n - 1)
    qcopy.wait()

    def send_own(c):
        blk = qblk(c, me)
        remote(blk, blk, send_sem.at[0], ql_sem.at[c], right).start()
        remote(blk, blk, send_sem.at[1], qr_sem.at[c], left).start()
        remote(blk, blk, send_sem.at[2], qp_sem.at[c], mate).start()

    def q_first(c):
        wait_on(qblk(c, left), ql_sem.at[c])
        wait_on(qblk(c, right), qr_sem.at[c])
        even = c % 2 == 0
        blk = qblk(c, jnp.where(even, left, right))
        remote(blk, blk, send_sem.at[3], qd_sem.at[c], jnp.where(even, right, left)).start()
        for j in (left, right):
            blk = qblk(c, j)
            remote(blk, blk, send_sem.at[2], qp_sem.at[c], mate).start()

    def q_second(c):
        blk = qblk(c, opp)
        wait_on(blk, qd_sem.at[c])
        remote(blk, blk, send_sem.at[2], qp_sem.at[c], mate).start()

    def q_third(c):
        wait_on(qall.at[pl.ds(c * G, G), pl.ds((1 - core) * half, half), :], qp_sem.at[c])

    def scores(c):
        for g in range(G):
            b = c * G + g
            ct = cbuf[b % RING]
            ct = jnp.concatenate([ct[i] for i in range(npage)], axis=1)
            s = lax.dot_general(qall[b], ct, (((1,), (0,)), ((), ())), preferred_element_type=jnp.float32)
            length = lens_ref[b] - me * npage
            posr = lax.broadcasted_iota(jnp.int32, (1, r), 1) * (n * npage)
            mask = jnp.concatenate([posr < length - i for i in range(npage)], axis=1)
            s = jnp.where(mask, s, -jnp.inf)
            m = jnp.max(s, axis=1, keepdims=True) * C2
            msafe = jnp.where(m == -jnp.inf, 0.0, m)
            p = jnp.exp2(s * C2 - msafe)
            l = jnp.sum(p, axis=1, keepdims=True)
            ps = b % PSLOT
            pbuf[ps] = p
            mbuf[ps] = m
            lse = jnp.where(l > 0.0, msafe + jnp.log2(jnp.where(l > 0.0, l, 1.0)), -jnp.inf)
            t = jnp.transpose(jnp.broadcast_to(lse, (heads, heads)))
            lse_all[me, b] = t[0:1]

    def product(c):
        for g in range(G):
            b = c * G + g
            rows = [lse_all[j, b] for j in range(n)]
            top = functools.reduce(jnp.maximum, rows)
            tot = functools.reduce(jnp.add, [jnp.exp2(z - top) for z in rows])
            big = top + jnp.log2(tot)
            bigc = jnp.transpose(jnp.broadcast_to(big, (heads, heads)))[:, 0:1]
            ps = b % PSLOT
            f = jnp.exp2(mbuf[ps] - bigc)
            a = (pbuf[ps] * f).astype(jnp.bfloat16)
            ct = cbuf[b % RING]
            ct = jnp.concatenate([ct[i, :lorav] for i in range(npage)], axis=1)
            if NT:
                obuf[b] = lax.dot_general(a, ct, (((1,), (1,)), ((), ())), preferred_element_type=jnp.float32)
            else:
                ot = lax.dot_general(ct, a, (((1,), (1,)), ((), ())), preferred_element_type=jnp.float32)
                obuf[b] = jnp.transpose(ot)

    def scores_wait(c):
        for g in range(G):
            cache_copy(c * G + g).wait()

    def product_wait(c):
        wait_on(lse_all.at[pl.ds(0, n - 1), pl.ds(c * G, G)], lse_sem.at[c])

    def scores_send(c):
        blk = lse_all.at[me, pl.ds(c * G, G)]
        for d in range(1, n):
            remote(blk, blk, send_sem.at[4], lse_sem.at[c], (me + d) % n).start()

    def product_send(c):
        bs = pl.ds(c * G, G)
        remote(obuf.at[bs, pl.ds((1 - core) * half, half)], xrecv.at[bs], send_sem.at[5], x_sem.at[c],
               mate).start()
        for g in range(G):
            b = c * G + g

            @pl.when(b + RING < nseq)
            def _():
                cache_copy(b + RING).start()

    def chip_sum(c):
        bs = pl.ds(c * G, G)
        wait_on(xrecv.at[bs], x_sem.at[c])
        snd[bs] = (obuf[bs, pl.ds(core * half, half)] + xrecv[bs]).astype(jnp.bfloat16)

        def part(j):
            return snd.at[bs, pl.ds((j // 2) * hl, hl)]

        even = c % 2 == 0
        remote(part(opp), relay_in.at[bs], send_sem.at[6], a_sem.at[c], jnp.where(even, right, left)).start()
        remote(part(right), o_in.at[0, bs], send_sem.at[6], ol_sem.at[c], right).start()
        remote(part(left), o_in.at[1, bs], send_sem.at[6], or_sem.at[c], left).start()

    def relay(c):
        bs = pl.ds(c * G, G)
        wait_on(relay_in.at[bs], a_sem.at[c])
        remote(relay_in.at[bs], o_in.at[2, bs], send_sem.at[7], od_sem.at[c],
               jnp.where(c % 2 == 0, right, left)).start()

    def final(c):
        bs = pl.ds(c * G, G)
        wait_on(o_in.at[0, bs], ol_sem.at[c])
        wait_on(o_in.at[1, bs], or_sem.at[c])
        wait_on(o_in.at[2, bs], od_sem.at[c])
        own = obuf[bs, pl.ds(row(me), hl)] + xrecv[bs, pl.ds(x * hl, hl)]
        o_ref[bs] = (own + o_in[0, bs].astype(jnp.float32) + o_in[1, bs].astype(jnp.float32)
                     + o_in[2, bs].astype(jnp.float32)).astype(o_ref.dtype)

    for c in range(AHEAD):
        send_own(c)

    def step(it, do_scores, do_product):
        def stage(f, d):
            @pl.when((it >= d) & (it < nc + d))
            def _():
                f(it - d)

        @pl.when(it + AHEAD < nc)
        def _():
            send_own(it + AHEAD)

        stage(q_first, 0)
        stage(q_second, D_Q2)
        stage(q_third, D_Q3)
        stage(chip_sum, D_CS)
        stage(relay, D_RL)
        stage(final, D_FI)
        if do_scores:
            scores_wait(it - D_SC)
        if do_product:
            product_wait(it - D_PR)
        if do_scores:
            scores(it - D_SC)
        if do_product:
            product(it - D_PR)
        if do_scores:
            scores_send(it - D_SC)
        if do_product:
            product_send(it - D_PR)

    def run(lo, hi, do_scores, do_product):
        @pl.loop(lo, hi)
        def _(it):
            step(it, do_scores, do_product)

    run(0, D_SC, False, False)
    run(D_SC, D_PR, True, False)
    run(D_PR, nc + D_SC, True, True)
    run(nc + D_SC, nc + D_PR, False, True)
    run(nc + D_PR, nc + D_FI, False, False)

    wait_on(qall.at[:, pl.ds(0, hl), :], send_sem.at[0])
    wait_on(qall.at[:, pl.ds(0, hl), :], send_sem.at[1])
    wait_on(qall.at[:, pl.ds(0, half), :], send_sem.at[2])
    wait_on(qall.at[:, pl.ds(0, hl), :], send_sem.at[3])
    wait_on(lse_all.at[pl.ds(0, n - 1)], send_sem.at[4])
    wait_on(xrecv, send_sem.at[5])
    wait_on(snd.at[:, pl.ds(0, (nx - 1) * hl)], send_sem.at[6])
    wait_on(relay_in, send_sem.at[7])


def solution(mesh):
    n = mesh.shape['dcp']

    def local(q, cache, lens):
        b, hl, k = q.shape
        r = cache.shape[1]
        page = cache.shape[3]
        lorav = k - ROPE
        ct = cache.reshape(b, r, page, k).transpose(0, 2, 3, 1)
        heads = n * hl
        half = heads // 2
        nc = b // G
        dma = pltpu.SemaphoreType.DMA
        return pl.pallas_call(
            functools.partial(kernel, n),
            out_shape=jax.ShapeDtypeStruct((b, hl, lorav), jnp.bfloat16),
            in_specs=[pl.BlockSpec(memory_space=pl.ANY), pl.BlockSpec(memory_space=pl.ANY),
                      pl.BlockSpec(memory_space=pltpu.SMEM)],
            out_specs=pl.BlockSpec(memory_space=pltpu.VMEM),
            scratch_shapes=[
                pltpu.VMEM((b, heads, k), jnp.bfloat16),
                pltpu.VMEM((RING, page, k, r), jnp.bfloat16),
                pltpu.VMEM((PSLOT, heads, r * page), jnp.float32),
                pltpu.VMEM((PSLOT, heads, 1), jnp.float32),
                pltpu.VMEM((n, b, 1, heads), jnp.float32),
                pltpu.VMEM((b, heads, lorav), jnp.float32),
                pltpu.VMEM((b, half, lorav), jnp.float32),
                pltpu.VMEM((b, half, lorav), jnp.bfloat16),
                pltpu.VMEM((b, hl, lorav), jnp.bfloat16),
                pltpu.VMEM((3, b, hl, lorav), jnp.bfloat16),
                dma((1,)), dma((RING,)), dma((8,)),
            ] + [dma((nc,))] * 10,
            compiler_params=pltpu.CompilerParams(
                collective_id=0, has_side_effects=True, vmem_limit_bytes=66_000_000),
        )(q, ct, lens)

    return jax.shard_map(local, mesh=mesh,
                         in_specs=(P('dp', 'dcp', None), P('dp', None, 'dcp', None, None), P('dp')),
                         out_specs=P('dp', 'dcp', None), check_vma=False)
```

```python
import functools

import jax
import jax.numpy as jnp
from jax import lax
from jax.experimental import pallas as pl
from jax.experimental.pallas import tpu as pltpu
from jax.sharding import PartitionSpec as P

ROPE = 64
QK_DIM = 192
C2 = QK_DIM ** -0.5 * 1.4426950408889634

G = 2
GQ = 2
AHEAD = 4
RING = 14
PSLOT = 8
LEAD = 3
EARLY = 2
D_Q2 = 4
D_Q3 = 6
D_SC = 6
D_PR = 8
D_CS = 10
D_RL = 14
D_FI = 19
NT = True


def kernel(n, q_hbm, c_hbm, lens_ref, o_ref, qall, cbuf, pbuf, abuf, mbuf, lse_own, lse_mate, lse_chip, lse_in, wt, obuf, xrecv, snd,
           relay_in, o_in, lsem, csem, send_sem, ql_sem, qr_sem, qd_sem, qp_sem, lse_sem, lc_sem, x_sem,
           a_sem, ol_sem, or_sem, od_sem):
    nseq, hl, k = q_hbm.shape
    npage, _, r = c_hbm.shape[1:]
    lorav = k - ROPE
    nx = n // 2
    half = nx * hl
    heads = n * hl
    nc = nseq // G
    nq = nseq // GQ

    me = lax.axis_index('dcp')
    x = lax.div(me, 2)
    core = lax.rem(me, 2)
    right = lax.rem(me + 2, n)
    left = lax.rem(me + n - 2, n)
    opp = lax.rem(me + 4, n)
    mate = me + 1 - 2 * core

    def row(j):
        return (lax.rem(j, 2) * nx + lax.div(j, 2)) * hl

    def remote(src, dst, ssem, rsem, dev):
        return pltpu.make_async_remote_copy(
            src_ref=src, dst_ref=dst, send_sem=ssem, recv_sem=rsem, device_id={'dcp': dev},
            device_id_type=pl.DeviceIdType.MESH)

    def wait_on(ref, sem):
        pltpu.make_async_copy(ref, ref, sem).wait()

    def cache_copy(b):
        s = lax.rem(b, RING)
        return pltpu.make_async_copy(c_hbm.at[b], cbuf.at[s], csem.at[s])

    def qblk(c, j):
        return qall.at[pl.ds(c * GQ, GQ), pl.ds(row(j), hl), :]

    qcopy = pltpu.make_async_copy(q_hbm, qall.at[:, pl.ds(row(me), hl), :], lsem.at[0])
    qcopy.start()
    for b in range(EARLY * G):
        cache_copy(b).start()

    barrier = pltpu.get_barrier_semaphore()
    for d in range(1, n):
        pl.semaphore_signal(barrier, inc=1, device_id={'dcp': lax.rem(me + d, n)},
                            device_id_type=pl.DeviceIdType.MESH)
    pl.semaphore_wait(barrier, n - 1)
    qcopy.wait()

    def send_own(c):
        blk = qblk(c, me)
        remote(blk, blk, send_sem.at[0], ql_sem.at[c], right).start()
        remote(blk, blk, send_sem.at[1], qr_sem.at[c], left).start()
        remote(blk, blk, send_sem.at[2], qp_sem.at[c], mate).start()

    def q_first(c):
        wait_on(qblk(c, left), ql_sem.at[c])
        wait_on(qblk(c, right), qr_sem.at[c])
        even = lax.rem(c, 2) == 0
        blk = qblk(c, jnp.where(even, left, right))
        remote(blk, blk, send_sem.at[3], qd_sem.at[c], jnp.where(even, right, left)).start()
        for j in (left, right):
            blk = qblk(c, j)
            remote(blk, blk, send_sem.at[2], qp_sem.at[c], mate).start()

    def q_second(c):
        blk = qblk(c, opp)
        wait_on(blk, qd_sem.at[c])
        remote(blk, blk, send_sem.at[2], qp_sem.at[c], mate).start()

    def q_third(c):
        wait_on(qall.at[pl.ds(c * GQ, GQ), pl.ds((1 - core) * half, half), :], qp_sem.at[c])

    def score_dot(c, g):
        b = c * G + g
        ct = cbuf[lax.rem(b, RING)]
        ct = jnp.concatenate([ct[i] for i in range(npage)], axis=1)
        return lax.dot_general(qall[b], ct, (((1,), (0,)), ((), ())), preferred_element_type=jnp.float32)

    def softmax(c, g, s):
        b = c * G + g
        length = lens_ref[b] - me * npage
        posr = lax.broadcasted_iota(jnp.int32, (1, r), 1) * (n * npage)
        mask = jnp.concatenate([posr < length - i for i in range(npage)], axis=1)
        s = jnp.where(mask, s, -jnp.inf)
        m = jnp.max(s, axis=1, keepdims=True) * C2
        msafe = jnp.where(m == -jnp.inf, 0.0, m)
        p = jnp.exp2(s * C2 - msafe)
        l = jnp.sum(p, axis=1, keepdims=True)
        ps = lax.rem(b, PSLOT)
        pbuf[ps] = p
        mbuf[ps] = m
        lse = jnp.where(l > 0.0, msafe + jnp.log2(jnp.where(l > 0.0, l, 1.0)), -jnp.inf)
        t = jnp.transpose(jnp.broadcast_to(lse, (heads, heads)))
        lse_own[b] = t[0:1]

    def weigh(c, g):
        b = c * G + g
        u, v = lse_own[b], lse_mate[b]
        top = jnp.maximum(u, v)
        top = jnp.where(top == -jnp.inf, 0.0, top)
        big = top + jnp.log2(jnp.exp2(u - top) + jnp.exp2(v - top))
        lse_chip[b] = big
        big = jnp.where(big == -jnp.inf, 0.0, big)
        bigc = jnp.transpose(jnp.broadcast_to(big, (heads, heads)))[:, 0:1]
        ps = lax.rem(b, PSLOT)
        f = jnp.exp2(mbuf[ps] - bigc)
        abuf[g] = (pbuf[ps] * f).astype(jnp.bfloat16)

    def product_dot(c, g):
        b = c * G + g
        ct = cbuf[lax.rem(b, RING)]
        ct = jnp.concatenate([ct[i, :lorav] for i in range(npage)], axis=1)
        if NT:
            obuf[b] = lax.dot_general(abuf[g], ct, (((1,), (1,)), ((), ())), preferred_element_type=jnp.float32)
        else:
            ot = lax.dot_general(ct, abuf[g], (((1,), (1,)), ((), ())), preferred_element_type=jnp.float32)
            obuf[b] = jnp.transpose(ot)

    def arithmetic(cs, cp, cc, cf):
        if cc is not None:
            bs = pl.ds(cc * G, G)
            snd[bs] = (obuf[bs, pl.ds(core * half, half)] + xrecv[bs]).astype(jnp.bfloat16)
        if cp is not None:
            for g in range(G):
                weigh(cp, g)
        for g in range(G):
            if cs is not None:
                s = score_dot(cs, g)
            if cp is not None:
                product_dot(cp, g)
            if cs is not None:
                softmax(cs, g, s)
        if cf is not None:
            final(cf)

    def scores_wait(c):
        for g in range(G):
            cache_copy(c * G + g).wait()

    def product_wait(c):
        wait_on(lse_mate.at[pl.ds(c * G, G)], lse_sem.at[c])

    def scores_send(c):
        bs = pl.ds(c * G, G)
        remote(lse_own.at[bs], lse_mate.at[bs], send_sem.at[4], lse_sem.at[c], mate).start()

    def product_send(c):
        bs = pl.ds(c * G, G)
        remote(obuf.at[bs, pl.ds((1 - core) * half, half)], xrecv.at[bs], send_sem.at[5], x_sem.at[c],
               mate).start()
        for i, j in enumerate((right, left, opp)):
            remote(lse_chip.at[bs], lse_in.at[i, bs], send_sem.at[8], lc_sem.at[c], j).start()

    def prefetch(c):
        for g in range(G):
            cache_copy(c * G + g).start()

    def chip_wait(c):
        wait_on(xrecv.at[pl.ds(c * G, G)], x_sem.at[c])

    def chip_send(c):
        bs = pl.ds(c * G, G)

        def part(j):
            return snd.at[bs, pl.ds(lax.div(j, 2) * hl, hl)]

        even = lax.rem(c, 2) == 0
        remote(part(opp), relay_in.at[bs], send_sem.at[6], a_sem.at[c], jnp.where(even, right, left)).start()
        remote(part(right), o_in.at[0, bs], send_sem.at[6], ol_sem.at[c], right).start()
        remote(part(left), o_in.at[1, bs], send_sem.at[6], or_sem.at[c], left).start()

    def relay(c):
        bs = pl.ds(c * G, G)
        wait_on(relay_in.at[bs], a_sem.at[c])
        remote(relay_in.at[bs], o_in.at[2, bs], send_sem.at[7], od_sem.at[c],
               jnp.where(lax.rem(c, 2) == 0, right, left)).start()

    def final_wait(c):
        bs = pl.ds(c * G, G)
        wait_on(o_in.at[0, bs], ol_sem.at[c])
        wait_on(o_in.at[1, bs], or_sem.at[c])
        wait_on(o_in.at[2, bs], od_sem.at[c])
        wait_on(lse_in.at[:, bs], lc_sem.at[c])

    def final(c):
        rows = []
        for g in range(G):
            b = c * G + g
            z = [lse_chip[b]] + [lse_in[i, b] for i in range(3)]
            top = functools.reduce(jnp.maximum, z)
            z = [jnp.exp2(y - top) for y in z]
            tot = functools.reduce(jnp.add, z)
            rows += [y / tot for y in z]
        wt[...] = jnp.transpose(jnp.concatenate(rows, axis=0))
        w = wt[pl.ds(row(me), hl), :]
        for g in range(G):
            b = c * G + g
            o = (obuf[b, pl.ds(row(me), hl)] + xrecv[b, pl.ds(x * hl, hl)]) * w[:, 4 * g:4 * g + 1]
            for i in range(3):
                o += o_in[i, b].astype(jnp.float32) * w[:, 4 * g + 1 + i:4 * g + 2 + i]
            o_ref[b] = o.astype(o_ref.dtype)

    for c in range(AHEAD):
        send_own(c)

    def step(it, live):
        def stage(f, d, count=nc, skip=0):
            @pl.when((it >= d + skip) & (it < count + d))
            def _():
                f(it - d)

        @pl.when(it + AHEAD < nq)
        def _():
            send_own(it + AHEAD)

        stage(prefetch, D_SC - LEAD, nc, EARLY)
        stage(q_first, 0, nq)
        stage(q_second, D_Q2, nq)
        stage(q_third, D_Q3, nq)
        stage(relay, D_RL)
        cs, cp, cc, cf = [it - d if on else None for d, on in zip((D_SC, D_PR, D_CS, D_FI), live)]
        if cs is not None:
            scores_wait(cs)
        if cp is not None:
            product_wait(cp)
        if cc is not None:
            chip_wait(cc)
        if cf is not None:
            final_wait(cf)
        arithmetic(cs, cp, cc, cf)
        if cs is not None:
            scores_send(cs)
        if cp is not None:
            product_send(cp)
        if cc is not None:
            chip_send(cc)

    marks = sorted({0} | {d + e for d in (D_SC, D_PR, D_CS, D_FI) for e in (0, nc)})
    for lo, hi in zip(marks, marks[1:]):
        live = [d <= lo < d + nc for d in (D_SC, D_PR, D_CS, D_FI)]

        @pl.loop(lo, hi)
        def _(it, live=live):
            step(it, live)

    wait_on(qall.at[:, pl.ds(0, hl), :], send_sem.at[0])
    wait_on(qall.at[:, pl.ds(0, hl), :], send_sem.at[1])
    wait_on(qall.at[:, pl.ds(0, half), :], send_sem.at[2])
    wait_on(qall.at[:, pl.ds(0, hl), :], send_sem.at[3])
    wait_on(lse_own, send_sem.at[4])
    wait_on(lse_in, send_sem.at[8])
    wait_on(xrecv, send_sem.at[5])
    wait_on(snd.at[:, pl.ds(0, (nx - 1) * hl)], send_sem.at[6])
    wait_on(relay_in, send_sem.at[7])


def solution(mesh):
    n = mesh.shape['dcp']

    def local(q, cache, lens):
        b, hl, k = q.shape
        r = cache.shape[1]
        page = cache.shape[3]
        lorav = k - ROPE
        ct = cache.reshape(b, r, page, k).transpose(0, 2, 3, 1)
        heads = n * hl
        half = heads // 2
        nc = b // G
        dma = pltpu.SemaphoreType.DMA
        return pl.pallas_call(
            functools.partial(kernel, n),
            out_shape=jax.ShapeDtypeStruct((b, hl, lorav), jnp.bfloat16),
            in_specs=[pl.BlockSpec(memory_space=pl.ANY), pl.BlockSpec(memory_space=pl.ANY),
                      pl.BlockSpec(memory_space=pltpu.SMEM)],
            out_specs=pl.BlockSpec(memory_space=pltpu.VMEM),
            scratch_shapes=[
                pltpu.VMEM((b, heads, k), jnp.bfloat16),
                pltpu.VMEM((RING, page, k, r), jnp.bfloat16),
                pltpu.VMEM((PSLOT, heads, r * page), jnp.float32),
                pltpu.VMEM((G, heads, r * page), jnp.bfloat16),
                pltpu.VMEM((PSLOT, heads, 1), jnp.float32),
                pltpu.VMEM((b, 1, heads), jnp.float32),
                pltpu.VMEM((b, 1, heads), jnp.float32),
                pltpu.VMEM((b, 1, heads), jnp.float32),
                pltpu.VMEM((3, b, 1, heads), jnp.float32),
                pltpu.VMEM((heads, 4 * G), jnp.float32),
                pltpu.VMEM((b, heads, lorav), jnp.float32),
                pltpu.VMEM((b, half, lorav), jnp.float32),
                pltpu.VMEM((b, half, lorav), jnp.bfloat16),
                pltpu.VMEM((b, hl, lorav), jnp.bfloat16),
                pltpu.VMEM((3, b, hl, lorav), jnp.bfloat16),
                dma((1,)), dma((RING,)), dma((9,)),
            ] + [dma((b // GQ,))] * 4 + [dma((nc,))] * 7,
            compiler_params=pltpu.CompilerParams(
                collective_id=0, has_side_effects=True, vmem_limit_bytes=66_000_000),
        )(q, ct, lens)

    return jax.shard_map(local, mesh=mesh,
                         in_specs=(P('dp', 'dcp', None), P('dp', None, 'dcp', None, None), P('dp')),
                         out_specs=P('dp', 'dcp', None), check_vma=False)
```

```python
import functools

import jax
import jax.numpy as jnp
from jax import lax
from jax.experimental import pallas as pl
from jax.experimental.pallas import tpu as pltpu
from jax.sharding import PartitionSpec as P

ROPE = 64
QK_DIM = 192
C2 = QK_DIM ** -0.5 * 1.4426950408889634

G = 2
AHEAD = 4
RING = 12
PSLOT = 8
LEAD = 3
EARLY = 2
D_Q2 = 4
D_Q3 = 6
D_SC = 6
D_PR = 8
D_CS = 10
D_RL = 14
D_FI = 19
NT = False


def kernel(n, q_hbm, c_hbm, lens_hbm, o_ref, lens_ref, qloc, qall, cbuf, pbuf, abuf, mbuf, lse_own, lse_mate, lse_chip, lse_in, wt, obuf, xrecv, snd,
           relay_in, o_in, lsem, csem, send_sem, ql_sem, qr_sem, qd_sem, qp_sem, lse_sem, lc_sem, x_sem,
           a_sem, ol_sem, or_sem, od_sem):
    nseq, hl, k = q_hbm.shape
    npage, _, r = c_hbm.shape[1:]
    lorav = k - ROPE
    nx = n // 2
    half = nx * hl
    heads = n * hl
    nc = nseq // G
    nq = nc

    me = lax.axis_index('dcp')
    x = lax.div(me, 2)
    core = lax.rem(me, 2)
    right = lax.rem(me + 2, n)
    left = lax.rem(me + n - 2, n)
    opp = lax.rem(me + 4, n)
    mate = me + 1 - 2 * core

    def row(j):
        return (lax.rem(j, 2) * nx + lax.div(j, 2)) * hl

    def remote(src, dst, ssem, rsem, dev):
        return pltpu.make_async_remote_copy(
            src_ref=src, dst_ref=dst, send_sem=ssem, recv_sem=rsem, device_id={'dcp': dev},
            device_id_type=pl.DeviceIdType.MESH)

    def wait_on(ref, sem):
        pltpu.make_async_copy(ref, ref, sem).wait()

    def cache_copy(b):
        s = lax.rem(b, RING)
        return pltpu.make_async_copy(c_hbm.at[b], cbuf.at[s], csem.at[s])

    def qblk(c, j):
        return qall.at[c, pl.ds(row(j), hl), :]

    qcopy = pltpu.make_async_copy(q_hbm, qloc, lsem.at[0])
    qcopy.start()
    lcopy = pltpu.make_async_copy(lens_hbm, lens_ref, lsem.at[1])
    lcopy.start()
    for b in range(EARLY * G):
        cache_copy(b).start()

    barrier = pltpu.get_barrier_semaphore()
    for d in range(1, n):
        pl.semaphore_signal(barrier, inc=1, device_id={'dcp': lax.rem(me + d, n)},
                            device_id_type=pl.DeviceIdType.MESH)
    qcopy.wait()
    lcopy.wait()
    for c in range(nq):
        u, v = qloc[2 * c], qloc[2 * c + 1]
        qall[c, pl.ds(row(me), hl), :] = jnp.concatenate(
            [u[:, :lorav], v[:, :lorav], u[:, lorav:], v[:, lorav:]], axis=1)
    pl.semaphore_wait(barrier, n - 1)

    def send_own(c):
        blk = qblk(c, me)
        remote(blk, blk, send_sem.at[0], ql_sem.at[c], right).start()
        remote(blk, blk, send_sem.at[1], qr_sem.at[c], left).start()
        remote(blk, blk, send_sem.at[2], qp_sem.at[c], mate).start()

    def q_first(c):
        wait_on(qblk(c, left), ql_sem.at[c])
        wait_on(qblk(c, right), qr_sem.at[c])
        even = lax.rem(c, 2) == 0
        blk = qblk(c, jnp.where(even, left, right))
        remote(blk, blk, send_sem.at[3], qd_sem.at[c], jnp.where(even, right, left)).start()
        for j in (left, right):
            blk = qblk(c, j)
            remote(blk, blk, send_sem.at[2], qp_sem.at[c], mate).start()

    def q_second(c):
        blk = qblk(c, opp)
        wait_on(blk, qd_sem.at[c])
        remote(blk, blk, send_sem.at[2], qp_sem.at[c], mate).start()

    def q_third(c):
        wait_on(qall.at[c, pl.ds((1 - core) * half, half), :], qp_sem.at[c])

    def score_dot(c, g):
        b = c * G + g
        ct = cbuf[lax.rem(b, RING)]
        ct = jnp.concatenate([ct[i] for i in range(npage)], axis=1)
        zero = jnp.zeros((k - lorav, ct.shape[1]), ct.dtype)
        ct = jnp.concatenate([ct, zero] if g == 0 else [ct[:lorav], zero, ct[lorav:]], axis=0)
        q = qall[c]
        q = jnp.concatenate([q[:, g * lorav:(g + 1) * lorav], q[:, 2 * lorav:]], axis=1)
        return lax.dot_general(q, ct, (((1,), (0,)), ((), ())), preferred_element_type=jnp.float32)

    def softmax(c, g, s):
        b = c * G + g
        length = lens_ref[b] - me * npage
        posr = lax.broadcasted_iota(jnp.int32, (1, r), 1) * (n * npage)
        mask = jnp.concatenate([posr < length - i for i in range(npage)], axis=1)
        s = jnp.where(mask, s, -jnp.inf)
        m = jnp.max(s, axis=1, keepdims=True) * C2
        msafe = jnp.where(m == -jnp.inf, 0.0, m)
        p = jnp.exp2(s * C2 - msafe)
        l = jnp.sum(p, axis=1, keepdims=True)
        ps = lax.rem(b, PSLOT)
        pbuf[ps] = p
        mbuf[ps] = m
        lse = jnp.where(l > 0.0, msafe + jnp.log2(jnp.where(l > 0.0, l, 1.0)), -jnp.inf)
        t = jnp.transpose(jnp.broadcast_to(lse, (heads, heads)))
        lse_own[b] = t[0:1]

    def weigh(c, g):
        b = c * G + g
        u, v = lse_own[b], lse_mate[b]
        top = jnp.maximum(u, v)
        top = jnp.where(top == -jnp.inf, 0.0, top)
        big = top + jnp.log2(jnp.exp2(u - top) + jnp.exp2(v - top))
        lse_chip[b] = big
        big = jnp.where(big == -jnp.inf, 0.0, big)
        bigc = jnp.transpose(jnp.broadcast_to(big, (heads, heads)))[:, 0:1]
        ps = lax.rem(b, PSLOT)
        f = jnp.exp2(mbuf[ps] - bigc)
        abuf[g] = (pbuf[ps] * f).astype(jnp.bfloat16)

    def product_dot(c, g):
        b = c * G + g
        ct = cbuf[lax.rem(b, RING)]
        ct = jnp.concatenate([ct[i, :lorav] for i in range(npage)], axis=1)
        if NT:
            obuf[b] = lax.dot_general(abuf[g], ct, (((1,), (1,)), ((), ())), preferred_element_type=jnp.float32)
        else:
            ot = lax.dot_general(ct, abuf[g], (((1,), (1,)), ((), ())), preferred_element_type=jnp.float32)
            obuf[b] = jnp.transpose(ot)

    def arithmetic(cs, cp, cc, cf):
        if cc is not None:
            bs = pl.ds(cc * G, G)
            snd[bs] = (obuf[bs, pl.ds(core * half, half)] + xrecv[bs]).astype(jnp.bfloat16)
        if cp is not None:
            for g in range(G):
                weigh(cp, g)
        for g in range(G):
            if cs is not None:
                s = score_dot(cs, g)
            if cp is not None:
                product_dot(cp, g)
            if cs is not None:
                softmax(cs, g, s)
        if cf is not None:
            final(cf)

    def scores_wait(c):
        for g in range(G):
            cache_copy(c * G + g).wait()

    def product_wait(c):
        wait_on(lse_mate.at[pl.ds(c * G, G)], lse_sem.at[c])

    def scores_send(c):
        bs = pl.ds(c * G, G)
        remote(lse_own.at[bs], lse_mate.at[bs], send_sem.at[4], lse_sem.at[c], mate).start()

    def product_send(c):
        bs = pl.ds(c * G, G)
        remote(obuf.at[bs, pl.ds((1 - core) * half, half)], xrecv.at[bs], send_sem.at[5], x_sem.at[c],
               mate).start()
        for i, j in enumerate((right, left, opp)):
            remote(lse_chip.at[bs], lse_in.at[i, bs], send_sem.at[8], lc_sem.at[c], j).start()

    def prefetch(c):
        for g in range(G):
            cache_copy(c * G + g).start()

    def chip_wait(c):
        wait_on(xrecv.at[pl.ds(c * G, G)], x_sem.at[c])

    def chip_send(c):
        bs = pl.ds(c * G, G)

        def part(j):
            return snd.at[bs, pl.ds(lax.div(j, 2) * hl, hl)]

        even = lax.rem(c, 2) == 0
        remote(part(opp), relay_in.at[bs], send_sem.at[6], a_sem.at[c], jnp.where(even, right, left)).start()
        remote(part(right), o_in.at[0, bs], send_sem.at[6], ol_sem.at[c], right).start()
        remote(part(left), o_in.at[1, bs], send_sem.at[6], or_sem.at[c], left).start()

    def relay(c):
        bs = pl.ds(c * G, G)
        wait_on(relay_in.at[bs], a_sem.at[c])
        remote(relay_in.at[bs], o_in.at[2, bs], send_sem.at[7], od_sem.at[c],
               jnp.where(lax.rem(c, 2) == 0, right, left)).start()

    def final_wait(c):
        bs = pl.ds(c * G, G)
        wait_on(o_in.at[0, bs], ol_sem.at[c])
        wait_on(o_in.at[1, bs], or_sem.at[c])
        wait_on(o_in.at[2, bs], od_sem.at[c])
        wait_on(lse_in.at[:, bs], lc_sem.at[c])

    def final(c):
        rows = []
        for g in range(G):
            b = c * G + g
            z = [lse_chip[b]] + [lse_in[i, b] for i in range(3)]
            top = functools.reduce(jnp.maximum, z)
            z = [jnp.exp2(y - top) for y in z]
            tot = functools.reduce(jnp.add, z)
            rows += [y / tot for y in z]
        wt[...] = jnp.transpose(jnp.concatenate(rows, axis=0))
        w = wt[pl.ds(row(me), hl), :]
        for g in range(G):
            b = c * G + g
            o = (obuf[b, pl.ds(row(me), hl)] + xrecv[b, pl.ds(x * hl, hl)]) * w[:, 4 * g:4 * g + 1]
            for i in range(3):
                o += o_in[i, b].astype(jnp.float32) * w[:, 4 * g + 1 + i:4 * g + 2 + i]
            o_ref[b] = o.astype(o_ref.dtype)

    for c in range(AHEAD):
        send_own(c)

    def step(it, live):
        def stage(f, d, count=nc, skip=0):
            @pl.when((it >= d + skip) & (it < count + d))
            def _():
                f(it - d)

        @pl.when(it + AHEAD < nq)
        def _():
            send_own(it + AHEAD)

        stage(prefetch, D_SC - LEAD, nc, EARLY)
        stage(q_first, 0, nq)
        stage(q_second, D_Q2, nq)
        stage(q_third, D_Q3, nq)
        stage(relay, D_RL)
        cs, cp, cc, cf = [it - d if on else None for d, on in zip((D_SC, D_PR, D_CS, D_FI), live)]
        if cs is not None:
            scores_wait(cs)
        if cp is not None:
            product_wait(cp)
        if cc is not None:
            chip_wait(cc)
        if cf is not None:
            final_wait(cf)
        arithmetic(cs, cp, cc, cf)
        if cs is not None:
            scores_send(cs)
        if cp is not None:
            product_send(cp)
        if cc is not None:
            chip_send(cc)

    marks = sorted({0} | {d + e for d in (D_SC, D_PR, D_CS, D_FI) for e in (0, nc)})
    for lo, hi in zip(marks, marks[1:]):
        live = [d <= lo < d + nc for d in (D_SC, D_PR, D_CS, D_FI)]

        @pl.loop(lo, hi)
        def _(it, live=live):
            step(it, live)

    wait_on(qall.at[:, pl.ds(0, hl), :], send_sem.at[0])
    wait_on(qall.at[:, pl.ds(0, hl), :], send_sem.at[1])
    wait_on(qall.at[:, pl.ds(0, half), :], send_sem.at[2])
    wait_on(qall.at[:, pl.ds(0, hl), :], send_sem.at[3])
    wait_on(lse_own, send_sem.at[4])
    wait_on(lse_in, send_sem.at[8])
    wait_on(xrecv, send_sem.at[5])
    wait_on(snd.at[:, pl.ds(0, (nx - 1) * hl)], send_sem.at[6])
    wait_on(relay_in, send_sem.at[7])


def solution(mesh):
    n = mesh.shape['dcp']

    def local(q, cache, lens):
        b, hl, k = q.shape
        r = cache.shape[1]
        page = cache.shape[3]
        lorav = k - ROPE
        ct = cache.reshape(b, r, page, k).transpose(0, 2, 3, 1)
        heads = n * hl
        half = heads // 2
        nc = b // G
        dma = pltpu.SemaphoreType.DMA
        return pl.pallas_call(
            functools.partial(kernel, n),
            out_shape=jax.ShapeDtypeStruct((b, hl, lorav), jnp.bfloat16),
            in_specs=[pl.BlockSpec(memory_space=pltpu.HBM), pl.BlockSpec(memory_space=pltpu.HBM),
                      pl.BlockSpec(memory_space=pltpu.HBM)],
            out_specs=pl.BlockSpec(memory_space=pltpu.VMEM),
            scratch_shapes=[
                pltpu.SMEM((b,), jnp.int32),
                pltpu.VMEM((b, hl, k), jnp.bfloat16),
                pltpu.VMEM((nc, heads, 2 * k), jnp.bfloat16),
                pltpu.VMEM((RING, page, k, r), jnp.bfloat16),
                pltpu.VMEM((PSLOT, heads, r * page), jnp.float32),
                pltpu.VMEM((G, heads, r * page), jnp.bfloat16),
                pltpu.VMEM((PSLOT, heads, 1), jnp.float32),
                pltpu.VMEM((b, 1, heads), jnp.float32),
                pltpu.VMEM((b, 1, heads), jnp.float32),
                pltpu.VMEM((b, 1, heads), jnp.float32),
                pltpu.VMEM((3, b, 1, heads), jnp.float32),
                pltpu.VMEM((heads, 4 * G), jnp.float32),
                pltpu.VMEM((b, heads, lorav), jnp.float32),
                pltpu.VMEM((b, half, lorav), jnp.float32),
                pltpu.VMEM((b, half, lorav), jnp.bfloat16),
                pltpu.VMEM((b, hl, lorav), jnp.bfloat16),
                pltpu.VMEM((3, b, hl, lorav), jnp.bfloat16),
                dma((2,)), dma((RING,)), dma((9,)),
            ] + [dma((nc,))] * 11,
            compiler_params=pltpu.CompilerParams(
                collective_id=0, has_side_effects=True, vmem_limit_bytes=56_000_000),
        )(q, ct, lens)

    return jax.shard_map(local, mesh=mesh,
                         in_specs=(P('dp', 'dcp', None), P('dp', None, 'dcp', None, None), P('dp')),
                         out_specs=P('dp', 'dcp', None), check_vma=False)
```

```python
import functools

import jax
import jax.numpy as jnp
from jax import lax
from jax.experimental import pallas as pl
from jax.experimental.pallas import tpu as pltpu
from jax.sharding import PartitionSpec as P

ROPE = 64
QK_DIM = 192
C2 = QK_DIM ** -0.5 * 1.4426950408889634

G = 2
AHEAD = 4
RING = 12
PSLOT = 8
LG = 4
LEAD = 3
EARLY = 2
D_Q2 = 4
D_Q3 = 6
D_SC = 6
D_PR = 8
D_CS = 10
D_RL = 15
D_FI = 20
NT = False


def kernel(n, q_hbm, c_hbm, lens_hbm, o_ref, lens_ref, qloc, qall, cbuf, pbuf, abuf, mbuf, lse_own, lse_mate, lse_chip, lse_in, wt, obuf, xrecv, snd,
           relay_in, o_in, lsem, csem, send_sem, ql_sem, qr_sem, qd_sem, qp_sem, lse_sem, lc_sem, x_sem,
           a_sem, ol_sem, or_sem, od_sem):
    nseq, hl, k = q_hbm.shape
    npage, _, r = c_hbm.shape[1:]
    lorav = k - ROPE
    nx = n // 2
    half = nx * hl
    heads = n * hl
    nc = nseq // G
    nq = nc

    me = lax.axis_index('dcp')
    x = lax.div(me, 2)
    core = lax.rem(me, 2)
    right = lax.rem(me + 2, n)
    left = lax.rem(me + n - 2, n)
    opp = lax.rem(me + 4, n)
    mate = me + 1 - 2 * core

    def row(j):
        return (lax.rem(j, 2) * nx + lax.div(j, 2)) * hl

    def remote(src, dst, ssem, rsem, dev):
        return pltpu.make_async_remote_copy(
            src_ref=src, dst_ref=dst, send_sem=ssem, recv_sem=rsem, device_id={'dcp': dev},
            device_id_type=pl.DeviceIdType.MESH)

    def wait_on(ref, sem):
        pltpu.make_async_copy(ref, ref, sem).wait()

    def cache_copy(b):
        s = lax.rem(b, RING)
        return pltpu.make_async_copy(c_hbm.at[b], cbuf.at[s], csem.at[s])

    def qblk(c, j):
        return qall.at[c, pl.ds(row(j), hl), :]

    qcopy = pltpu.make_async_copy(q_hbm, qloc, lsem.at[0])
    qcopy.start()
    lcopy = pltpu.make_async_copy(lens_hbm, lens_ref, lsem.at[1])
    lcopy.start()
    for b in range(EARLY * G):
        cache_copy(b).start()

    barrier = pltpu.get_barrier_semaphore()
    for d in range(1, n):
        pl.semaphore_signal(barrier, inc=1, device_id={'dcp': lax.rem(me + d, n)},
                            device_id_type=pl.DeviceIdType.MESH)
    qcopy.wait()
    lcopy.wait()
    for c in range(nq):
        u, v = qloc[2 * c], qloc[2 * c + 1]
        qall[c, pl.ds(row(me), hl), :] = jnp.concatenate(
            [u[:, :lorav], v[:, :lorav], u[:, lorav:], v[:, lorav:]], axis=1)
    pl.semaphore_wait(barrier, n - 1)

    def send_own(c):
        blk = qblk(c, me)
        remote(blk, blk, send_sem.at[0], ql_sem.at[c], right).start()
        remote(blk, blk, send_sem.at[1], qr_sem.at[c], left).start()
        remote(blk, blk, send_sem.at[2], qp_sem.at[c], mate).start()

    def q_first(c):
        wait_on(qblk(c, left), ql_sem.at[c])
        wait_on(qblk(c, right), qr_sem.at[c])
        even = lax.rem(c, 2) == 0
        blk = qblk(c, jnp.where(even, left, right))
        remote(blk, blk, send_sem.at[3], qd_sem.at[c], jnp.where(even, right, left)).start()
        for j in (left, right):
            blk = qblk(c, j)
            remote(blk, blk, send_sem.at[2], qp_sem.at[c], mate).start()

    def q_second(c):
        blk = qblk(c, opp)
        wait_on(blk, qd_sem.at[c])
        remote(blk, blk, send_sem.at[2], qp_sem.at[c], mate).start()

    def q_third(c):
        wait_on(qall.at[c, pl.ds((1 - core) * half, half), :], qp_sem.at[c])

    def score_dot(c, g):
        b = c * G + g
        ct = cbuf[lax.rem(b, RING)]
        ct = jnp.concatenate([ct[i] for i in range(npage)], axis=1)
        zero = jnp.zeros((k - lorav, ct.shape[1]), ct.dtype)
        ct = jnp.concatenate([ct, zero] if g == 0 else [ct[:lorav], zero, ct[lorav:]], axis=0)
        q = qall[c]
        q = jnp.concatenate([q[:, g * lorav:(g + 1) * lorav], q[:, 2 * lorav:]], axis=1)
        return lax.dot_general(q, ct, (((1,), (0,)), ((), ())), preferred_element_type=jnp.float32)

    def softmax(c, g, s):
        b = c * G + g
        length = lens_ref[b] - me * npage
        posr = lax.broadcasted_iota(jnp.int32, (1, r), 1) * (n * npage)
        mask = jnp.concatenate([posr < length - i for i in range(npage)], axis=1)
        s = jnp.where(mask, s, -jnp.inf)
        m = jnp.max(s, axis=1, keepdims=True) * C2
        msafe = jnp.where(m == -jnp.inf, 0.0, m)
        p = jnp.exp2(s * C2 - msafe)
        l = jnp.sum(p, axis=1, keepdims=True)
        ps = lax.rem(b, PSLOT)
        pbuf[ps] = p
        mbuf[ps] = m
        lse = jnp.where(l > 0.0, msafe + jnp.log2(jnp.where(l > 0.0, l, 1.0)), -jnp.inf)
        t = jnp.transpose(jnp.broadcast_to(lse, (heads, heads)))
        lse_own[b] = t[0:1]

    def weigh(c, g):
        b = c * G + g
        u, v = lse_own[b], lse_mate[b]
        top = jnp.maximum(u, v)
        top = jnp.where(top == -jnp.inf, 0.0, top)
        big = top + jnp.log2(jnp.exp2(u - top) + jnp.exp2(v - top))
        whole = big
        big = jnp.where(big == -jnp.inf, 0.0, big)
        bigc = jnp.transpose(jnp.broadcast_to(big, (heads, heads)))[:, 0:1]
        ps = lax.rem(b, PSLOT)
        f = jnp.exp2(mbuf[ps] - bigc)
        abuf[g] = (pbuf[ps] * f).astype(jnp.bfloat16)
        return whole

    def product_dot(c, g):
        b = c * G + g
        ct = cbuf[lax.rem(b, RING)]
        ct = jnp.concatenate([ct[i, :lorav] for i in range(npage)], axis=1)
        if NT:
            obuf[b] = lax.dot_general(abuf[g], ct, (((1,), (1,)), ((), ())), preferred_element_type=jnp.float32)
        else:
            ot = lax.dot_general(ct, abuf[g], (((1,), (1,)), ((), ())), preferred_element_type=jnp.float32)
            obuf[b] = jnp.transpose(ot)

    def arithmetic(cs, cp, cc, cf):
        if cc is not None:
            bs = pl.ds(cc * G, G)
            snd[bs] = (obuf[bs, pl.ds(core * half, half)] + xrecv[bs]).astype(jnp.bfloat16)
        if cp is not None:
            u, v = [weigh(cp, g) for g in range(G)]
            u = jnp.where(core == 0, u, jnp.roll(u, half, axis=1))
            v = jnp.where(core == 0, jnp.roll(v, half, axis=1), v)
            lane = lax.broadcasted_iota(jnp.int32, (1, heads), 1)
            lse_chip[cp] = jnp.where(lane < half, u, v)
        for g in range(G):
            if cs is not None:
                s = score_dot(cs, g)
            if cp is not None:
                product_dot(cp, g)
            if cs is not None:
                softmax(cs, g, s)
        if cf is not None:
            final(cf)

    def scores_wait(c):
        for g in range(G):
            cache_copy(c * G + g).wait()

    def product_wait(c):
        wait_on(lse_mate.at[pl.ds(c * G, G)], lse_sem.at[c])

    def scores_send(c):
        bs = pl.ds(c * G, G)
        remote(lse_own.at[bs], lse_mate.at[bs], send_sem.at[4], lse_sem.at[c], mate).start()

    def product_send(c):
        bs = pl.ds(c * G, G)
        remote(obuf.at[bs, pl.ds((1 - core) * half, half)], xrecv.at[bs], send_sem.at[5], x_sem.at[c],
               mate).start()

        @pl.when(lax.rem(c, LG) == LG - 1)
        def _():
            cs = pl.ds(c - (LG - 1), LG)
            for i, j in enumerate((right, left, opp)):
                remote(lse_chip.at[cs], lse_in.at[i, cs], send_sem.at[8], lc_sem.at[lax.div(c, LG)], j).start()

    def prefetch(c):
        for g in range(G):
            cache_copy(c * G + g).start()

    def chip_wait(c):
        wait_on(xrecv.at[pl.ds(c * G, G)], x_sem.at[c])

    def chip_send(c):
        bs = pl.ds(c * G, G)

        def part(j):
            return snd.at[bs, pl.ds(lax.div(j, 2) * hl, hl)]

        remote(part(opp), relay_in.at[bs], send_sem.at[6], a_sem.at[c], onward(c)).start()
        remote(part(right), o_in.at[0, bs], send_sem.at[6], ol_sem.at[c], right).start()
        remote(part(left), o_in.at[1, bs], send_sem.at[6], or_sem.at[c], left).start()

    def onward(c):
        return jnp.where(lax.rem(c, 2) == 0, right, left)

    def relay(c):
        bs = pl.ds(c * G, G)
        wait_on(relay_in.at[bs], a_sem.at[c])
        remote(relay_in.at[bs], o_in.at[2, bs], send_sem.at[7], od_sem.at[c], onward(c)).start()

    def final_wait(c):
        bs = pl.ds(c * G, G)
        wait_on(o_in.at[0, bs], ol_sem.at[c])
        wait_on(o_in.at[1, bs], or_sem.at[c])
        wait_on(o_in.at[2, bs], od_sem.at[c])

        @pl.when(lax.rem(c, LG) == 0)
        def _():
            wait_on(lse_in.at[:, pl.ds(c, LG)], lc_sem.at[lax.div(c, LG)])

    def final(c):
        z = [lse_chip[c]] + [lse_in[i, c] for i in range(3)]
        top = functools.reduce(jnp.maximum, z)
        z = [jnp.exp2(y - top) for y in z]
        tot = functools.reduce(jnp.add, z)
        wt[...] = jnp.transpose(jnp.concatenate([y / tot for y in z + z], axis=0))
        for g in range(G):
            b = c * G + g
            w = wt[pl.ds(g * half + x * hl, hl), :]
            o = (obuf[b, pl.ds(row(me), hl)] + xrecv[b, pl.ds(x * hl, hl)]) * w[:, 0:1]
            for i in range(3):
                o += o_in[i, b].astype(jnp.float32) * w[:, 1 + i:2 + i]
            o_ref[b] = o.astype(o_ref.dtype)

    for c in range(AHEAD):
        send_own(c)

    def step(it, live):
        def stage(f, d, count=nc, skip=0):
            @pl.when((it >= d + skip) & (it < count + d))
            def _():
                f(it - d)

        @pl.when(it + AHEAD < nq)
        def _():
            send_own(it + AHEAD)

        stage(prefetch, D_SC - LEAD, nc, EARLY)
        stage(q_first, 0, nq)
        stage(q_second, D_Q2, nq)
        stage(q_third, D_Q3, nq)
        stage(relay, D_RL)
        cs, cp, cc, cf = [it - d if on else None for d, on in zip((D_SC, D_PR, D_CS, D_FI), live)]
        if cs is not None:
            scores_wait(cs)
        if cp is not None:
            product_wait(cp)
        if cc is not None:
            chip_wait(cc)
        if cf is not None:
            final_wait(cf)
        arithmetic(cs, cp, cc, cf)
        if cs is not None:
            scores_send(cs)
        if cp is not None:
            product_send(cp)
        if cc is not None:
            chip_send(cc)

    marks = sorted({0} | {d + e for d in (D_SC, D_PR, D_CS, D_FI) for e in (0, nc)})
    for lo, hi in zip(marks, marks[1:]):
        live = [d <= lo < d + nc for d in (D_SC, D_PR, D_CS, D_FI)]

        @pl.loop(lo, hi)
        def _(it, live=live):
            step(it, live)

    wait_on(qall.at[:, pl.ds(0, hl), :], send_sem.at[0])
    wait_on(qall.at[:, pl.ds(0, hl), :], send_sem.at[1])
    wait_on(qall.at[:, pl.ds(0, half), :], send_sem.at[2])
    wait_on(qall.at[:, pl.ds(0, hl), :], send_sem.at[3])
    wait_on(lse_own, send_sem.at[4])
    wait_on(lse_in, send_sem.at[8])
    wait_on(xrecv, send_sem.at[5])
    wait_on(snd.at[:, pl.ds(0, (nx - 1) * hl)], send_sem.at[6])
    wait_on(relay_in, send_sem.at[7])


def solution(mesh):
    n = mesh.shape['dcp']

    def local(q, cache, lens):
        b, hl, k = q.shape
        r = cache.shape[1]
        page = cache.shape[3]
        lorav = k - ROPE
        ct = cache.reshape(b, r, page, k).transpose(0, 2, 3, 1)
        heads = n * hl
        half = heads // 2
        nc = b // G
        dma = pltpu.SemaphoreType.DMA
        return pl.pallas_call(
            functools.partial(kernel, n),
            out_shape=jax.ShapeDtypeStruct((b, hl, lorav), jnp.bfloat16),
            in_specs=[pl.BlockSpec(memory_space=pltpu.HBM), pl.BlockSpec(memory_space=pltpu.HBM),
                      pl.BlockSpec(memory_space=pltpu.HBM)],
            out_specs=pl.BlockSpec(memory_space=pltpu.VMEM),
            scratch_shapes=[
                pltpu.SMEM((b,), jnp.int32),
                pltpu.VMEM((b, hl, k), jnp.bfloat16),
                pltpu.VMEM((nc, heads, 2 * k), jnp.bfloat16),
                pltpu.VMEM((RING, page, k, r), jnp.bfloat16),
                pltpu.VMEM((PSLOT, heads, r * page), jnp.float32),
                pltpu.VMEM((G, heads, r * page), jnp.bfloat16),
                pltpu.VMEM((PSLOT, heads, 1), jnp.float32),
                pltpu.VMEM((b, 1, heads), jnp.float32),
                pltpu.VMEM((b, 1, heads), jnp.float32),
                pltpu.VMEM((nc, 1, heads), jnp.float32),
                pltpu.VMEM((3, nc, 1, heads), jnp.float32),
                pltpu.VMEM((heads, 8), jnp.float32),
                pltpu.VMEM((b, heads, lorav), jnp.float32),
                pltpu.VMEM((b, half, lorav), jnp.float32),
                pltpu.VMEM((b, half, lorav), jnp.bfloat16),
                pltpu.VMEM((b, hl, lorav), jnp.bfloat16),
                pltpu.VMEM((3, b, hl, lorav), jnp.bfloat16),
                dma((2,)), dma((RING,)), dma((9,)),
            ] + [dma((nc,))] * 11,
            compiler_params=pltpu.CompilerParams(
                collective_id=0, has_side_effects=True, vmem_limit_bytes=56_000_000),
        )(q, ct, lens)

    return jax.shard_map(local, mesh=mesh,
                         in_specs=(P('dp', 'dcp', None), P('dp', None, 'dcp', None, None), P('dp')),
                         out_specs=P('dp', 'dcp', None), check_vma=False)
```
